32 devices in a mesh: dp: 8 (over y, x, core), tensor: 4 (over z).
Axes of the slice: x: 2, y: 2, z: 4, core: 2. Of those that a mesh axis runs over, the one named last changes fastest.
Arguments:
- tokens_in: bfloat16 [8192, 1536], P('dp'), may hold values from -6 to 6
- doc_ids: int32 [8192], replicated, may hold values from 0 to 3, never falling along the last dimension, each value on 1 to 4096 neighbouring positions
- out_grad: bfloat16 [8192, 1536], P('dp'), may hold values from -6 to 6
- norm_gains: bfloat16 [2, 1536], replicated, may hold values from 0.5 to 1.5
- conv_taps: bfloat16 [3, 1536], P(None, 'tensor'), may hold values from -3.5 to 3.5
- stream_weight: bfloat16 [3, 1536, 1536], P(None, None, 'tensor'), may hold values from -0.15625 to 0.15625
- mixer_weight: bfloat16 [1536, 1536], P('tensor'), may hold values from -0.15625 to 0.15625
- hidden_weight: bfloat16 [2, 1536, 6912], P(None, None, 'tensor'), may hold values from -0.15625 to 0.15625
- down_weight: bfloat16 [6912, 1536], P('tensor'), may hold values from -0.078125 to 0.078125
- gains_first: float32 [2, 1536], replicated, may hold values from -0.0009336855 to 0.0009336855
- gains_second: float32 [2, 1536], replicated, may hold values from 7.2647386e-09 to 7.264739e-08
- taps_first: float32 [3, 1536], P(None, 'tensor'), may hold values from -0.0009336855 to 0.0009336855
- taps_second: float32 [3, 1536], P(None, 'tensor'), may hold values from 7.2647386e-09 to 7.264739e-08
- stream_first: float32 [3, 1536, 1536], P(None, 'dp', 'tensor'), may hold values from -0.0009336855 to 0.0009336855
- stream_second: float32 [3, 1536, 1536], P(None, 'dp', 'tensor'), may hold values from 7.2647386e-09 to 7.264739e-08
- mixer_first: float32 [1536, 1536], P('tensor', 'dp'), may hold values from -0.0009336855 to 0.0009336855
- mixer_second: float32 [1536, 1536], P('tensor', 'dp'), may hold values from 7.2647386e-09 to 7.264739e-08
- hidden_first: float32 [2, 1536, 6912], P(None, 'dp', 'tensor'), may hold values from -0.0009336855 to 0.0009336855
- hidden_second: float32 [2, 1536, 6912], P(None, 'dp', 'tensor'), may hold values from 7.2647386e-09 to 7.264739e-08
- down_first: float32 [6912, 1536], P('tensor', 'dp'), may hold values from -0.0009336855 to 0.0009336855
- down_second: float32 [6912, 1536], P('tensor', 'dp'), may hold values from 7.2647386e-09 to 7.264739e-08
Outputs:
- block_out: bfloat16 [8192, 1536], P('dp')
- input_grad: float32 [8192, 1536], P('dp')
- grad_norm: float32 [], replicated
- gains_grad: float32 [2, 1536], replicated
- gains_first_next: float32 [2, 1536], replicated
- gains_second_next: float32 [2, 1536], replicated
- gains_step: float32 [2, 1536], replicated
- taps_grad: float32 [3, 1536], P(None, 'tensor')
- taps_first_next: float32 [3, 1536], P(None, 'tensor')
- taps_second_next: float32 [3, 1536], P(None, 'tensor')
- taps_step: float32 [3, 1536], P(None, 'tensor')
- stream_grad: float32 [3, 1536, 1536], P(None, 'dp', 'tensor')
- stream_first_next: float32 [3, 1536, 1536], P(None, 'dp', 'tensor')
- stream_second_next: float32 [3, 1536, 1536], P(None, 'dp', 'tensor')
- stream_step: float32 [3, 1536, 1536], P(None, 'dp', 'tensor')
- mixer_grad: float32 [1536, 1536], P('tensor', 'dp')
- mixer_first_next: float32 [1536, 1536], P('tensor', 'dp')
- mixer_second_next: float32 [1536, 1536], P('tensor', 'dp')
- mixer_step: float32 [1536, 1536], P('tensor', 'dp')
- hidden_grad: float32 [2, 1536, 6912], P(None, 'dp', 'tensor')
- hidden_first_next: float32 [2, 1536, 6912], P(None, 'dp', 'tensor')
- hidden_second_next: float32 [2, 1536, 6912], P(None, 'dp', 'tensor')
- hidden_step: float32 [2, 1536, 6912], P(None, 'dp', 'tensor')
- down_grad: float32 [6912, 1536], P('tensor', 'dp')
- down_first_next: float32 [6912, 1536], P('tensor', 'dp')
- down_second_next: float32 [6912, 1536], P('tensor', 'dp')
- down_step: float32 [6912, 1536], P('tensor', 'dp')
The draws below stay inside these ranges and needn't reach their ends.
Inputs may be any that keep to these rules, and one draw needn't show every extreme that they name: `doc_ids`: document ids never fall along the tokens; each document has 1 to 4096 tokens, and one has exactly 4096.
All inputs are finite; a program needn't handle non-finite values.
Results may differ from the reference program's by a relative error of at most 0.01.
The reference program's roundings to bfloat16 on the way count: a program that leaves them out, or rounds other values in their place, can miss the bound.
Values may be sent and summed in bfloat16 or wider, within the bound.
A program may use at most 256 MiB of HBM per device.

```python
import math
import jax
import jax.numpy as jnp
import numpy as np
from jax import lax

D = 1536
FF = 6912
KERNEL = 3
TOKENS = 8192
DOC_MOST = 4096
DOCS = 4
PARAMS = 41295360


def levels(stream_key, dims, cuts, smallest, largest):
    gain, own = 1.0, jax.random.fold_in(stream_key, 6)
    for position, blocks in cuts:
        draws = jnp.exp(jax.random.uniform(jax.random.fold_in(own, position), (blocks,), jnp.float32, smallest / len(cuts), largest / len(cuts)))
        gain = gain * jnp.repeat(draws, dims[position] // blocks).reshape([-1 if axis == position else 1 for axis in range(len(dims))])
    return gain


def length_profile(amount, total, most, lean):
    portions = [(1 << 20) // math.isqrt(rank ** lean) + 1 for rank in range(2, amount + 1)]
    surplus, given = total - most - (amount - 1), [1] * (amount - 1)
    while surplus > 0:
        movable = [i for i in range(amount - 1) if given[i] < most]
        mass, left = sum([portions[i] for i in movable]), surplus
        for i in movable:
            more = min(most - given[i], max(1, left * portions[i] // mass), surplus)
            given[i] = given[i] + more
            surplus = surplus - more
    return np.array([most] + given)


def uneven_parts(stream_key, count, total, reach, slope):
    if count == 2:
        one = jax.random.randint(stream_key, (), max(1, total - reach), min(reach, total - 1) + 1)
        return jnp.stack([one, total - one])
    tallies = jnp.asarray(length_profile(count, total, reach, slope), jnp.int32)
    couples = (count - 1) // 2
    donor, taker = tallies[1:1 + 2 * couples:2], tallies[2:2 + 2 * couples:2]
    margin = jnp.minimum(donor - 1, reach - taker)
    moved = jax.random.randint(jax.random.fold_in(stream_key, 1), (couples,), 0, 1 << 20) % (margin + 1)
    tallies = tallies.at[1:1 + 2 * couples:2].set(donor - moved).at[2:2 + 2 * couples:2].set(taker + moved)
    return tallies[jax.random.permutation(jax.random.fold_in(stream_key, 2), count)]


def normal_values(key, shape, scale, limit, shards=(), held_as=jnp.bfloat16):
    factor_of = levels(key, shape, shards, -0.22, 0.18) if shards else 1.0
    drawn = jax.random.normal(key, shape, jnp.float32) * scale * factor_of
    return jnp.minimum(jnp.maximum(drawn, -limit), limit).astype(held_as)


def setup_inputs(seed: int = 0) -> dict:
    keys = jax.random.split(jax.random.key(seed), 22)
    tokens_in = normal_values(keys[0], (TOKENS, D), 1.0, 6.0, ((0, 8),))
    doc_ids = jnp.searchsorted(jnp.cumsum(uneven_parts(keys[1], DOCS, TOKENS, DOC_MOST, 1)), jnp.arange(TOKENS), side="right").astype(jnp.int32)
    out_grad = normal_values(keys[2], (TOKENS, D), 1.0, 6.0, ((0, 8),))
    norm_gains = jnp.clip(1.0 + 0.1 * jax.random.normal(keys[3], (2, D), jnp.float32), 0.5, 1.5).astype(jnp.bfloat16)
    conv_taps = normal_values(keys[4], (KERNEL, D), KERNEL ** -0.5, 3.5, ((1, 4),))
    stream_weight = normal_values(keys[5], (3, D, D), D ** -0.5, 0.15625, ((2, 4),))
    mixer_weight = normal_values(keys[6], (D, D), D ** -0.5, 0.15625, ((0, 4),))
    hidden_weight = normal_values(keys[7], (2, D, FF), D ** -0.5, 0.15625, ((2, 4),))
    down_weight = normal_values(keys[8], (FF, D), FF ** -0.5, 0.078125, ((0, 4),))
    gains_first = normal_values(keys[9], (2, D), (PARAMS ** -0.5), 0.0009336855, (), jnp.float32)
    gains_second = jnp.clip(jnp.exp(jax.random.uniform(keys[10], (2, D), jnp.float32, math.log(7.264738588474984e-09), math.log(7.26473885492851e-08))), 7.264738588474984e-09, 7.26473885492851e-08)
    taps_first = normal_values(keys[11], (KERNEL, D), (PARAMS ** -0.5), 0.0009336855, ((1, 4),), jnp.float32)
    taps_second = jnp.clip(jnp.exp(math.log(7.26473885492851e-08) - 2.3025851 * jax.random.uniform(keys[12], (KERNEL, D), jnp.float32) ** levels(keys[12], (KERNEL, D), ((1, 4),), -0.2, 0.2)), 7.264738588474984e-09, 7.26473885492851e-08)
    stream_first = normal_values(keys[13], (3, D, D), (PARAMS ** -0.5), 0.0009336855, ((1, 8), (2, 4)), jnp.float32)
    stream_second = jnp.clip(jnp.exp(math.log(7.26473885492851e-08) - 2.3025851 * jax.random.uniform(keys[14], (3, D, D), jnp.float32) ** levels(keys[14], (3, D, D), ((1, 8), (2, 4)), -0.2, 0.2)), 7.264738588474984e-09, 7.26473885492851e-08)
    mixer_first = normal_values(keys[15], (D, D), (PARAMS ** -0.5), 0.0009336855, ((0, 4), (1, 8)), jnp.float32)
    mixer_second = jnp.clip(jnp.exp(math.log(7.26473885492851e-08) - 2.3025851 * jax.random.uniform(keys[16], (D, D), jnp.float32) ** levels(keys[16], (D, D), ((0, 4), (1, 8)), -0.2, 0.2)), 7.264738588474984e-09, 7.26473885492851e-08)
    hidden_first = normal_values(keys[17], (2, D, FF), (PARAMS ** -0.5), 0.0009336855, ((1, 8), (2, 4)), jnp.float32)
    hidden_second = jnp.clip(jnp.exp(math.log(7.26473885492851e-08) - 2.3025851 * jax.random.uniform(keys[18], (2, D, FF), jnp.float32) ** levels(keys[18], (2, D, FF), ((1, 8), (2, 4)), -0.2, 0.2)), 7.264738588474984e-09, 7.26473885492851e-08)
    down_first = normal_values(keys[19], (FF, D), (PARAMS ** -0.5), 0.0009336855, ((0, 4), (1, 8)), jnp.float32)
    down_second = jnp.clip(jnp.exp(math.log(7.26473885492851e-08) - 2.3025851 * jax.random.uniform(keys[20], (FF, D), jnp.float32) ** levels(keys[20], (FF, D), ((0, 4), (1, 8)), -0.2, 0.2)), 7.264738588474984e-09, 7.26473885492851e-08)
    return {"tokens_in": tokens_in, "doc_ids": doc_ids, "out_grad": out_grad, "norm_gains": norm_gains, "conv_taps": conv_taps, "stream_weight": stream_weight, "mixer_weight": mixer_weight, "hidden_weight": hidden_weight, "down_weight": down_weight, "gains_first": gains_first, "gains_second": gains_second, "taps_first": taps_first, "taps_second": taps_second, "stream_first": stream_first, "stream_second": stream_second, "mixer_first": mixer_first, "mixer_second": mixer_second, "hidden_first": hidden_first, "hidden_second": hidden_second, "down_first": down_first, "down_second": down_second}


HIGHEST_PRECISION = lax.Precision.HIGHEST
EPS_NORM = 1e-05
LEARN_RATE = 0.02
BETA_FIRST = 0.5
BETA_SECOND = 0.5
CORRECTION = 1.0 - 0.5 ** 3
ADAM_EPS = 1e-08
DECAY_RATE = 0.1
CLIP_NORM = 1.0

@jax.custom_vjp
def low(v):
    return lax.optimization_barrier(v.astype(jnp.bfloat16)).astype(jnp.float32)

@jax.custom_vjp
def low_back(v):
    return v

def low_keep(v):
    return (low(v), None)

def low_pass(kept, grad):
    return (grad,)

def back_keep(v):
    return (v, None)

def back_low(kept, grad):
    return (low(grad),)
low.defvjp(low_keep, low_pass)
low_back.defvjp(back_keep, back_low)

def rms_scale(values):
    return lax.rsqrt(lax.optimization_barrier(jnp.mean(values * values, axis=-1, keepdims=True)) + EPS_NORM)

def doc_valid(doc_ids, offset):
    earlier = jnp.concatenate([jnp.full((offset,), -1, jnp.int32), doc_ids[:doc_ids.shape[0] - offset]])
    return (earlier == doc_ids).astype(jnp.float32)[:, None]

def shift_down(values, offset):
    filler = jnp.zeros((offset, values.shape[1]), jnp.float32)
    return jnp.concatenate([filler, values[:values.shape[0] - offset]], 0)

def layer(tokens, norm_gains, conv_taps, stream_weight, mixer_weight, hidden_weight, down_weight, valid):
    normal_one = tokens * rms_scale(tokens)
    normed_one = low(normal_one * norm_gains[0])
    streams = jnp.einsum('td,sdc->stc', normed_one, stream_weight, precision=HIGHEST_PRECISION)
    gate_b = low_back(streams[0])
    gate_c = low_back(streams[1])
    values = low_back(streams[2])
    product = low(gate_b * values)
    mixed = conv_taps[0] * product
    for offset in range(1, conv_taps.shape[0]):
        mixed = mixed + conv_taps[offset] * shift_down(product, offset) * valid[offset]
    conv_out = low_back(mixed)
    gated = low(gate_c * conv_out)
    branch = low_back(jnp.dot(gated, mixer_weight, precision=HIGHEST_PRECISION))
    middle = tokens + branch
    normed_two = low(middle * rms_scale(middle) * norm_gains[1])
    hidden = jnp.einsum('td,sdf->stf', normed_two, hidden_weight, precision=HIGHEST_PRECISION)
    gate_h = low_back(hidden[0])
    up_h = low_back(hidden[1])
    active = low(gate_h * jax.nn.sigmoid(gate_h) * up_h)
    return middle + jnp.dot(active, down_weight, precision=HIGHEST_PRECISION)

def adam_step(master, gradient, first_moment, second_moment, factor, decay):
    clipped = gradient * factor
    first_next = BETA_FIRST * first_moment + (1.0 - BETA_FIRST) * clipped
    second_next = BETA_SECOND * second_moment + (1.0 - BETA_SECOND) * clipped * clipped
    change = -LEARN_RATE * (first_next / CORRECTION / (jnp.sqrt(second_next / CORRECTION) + ADAM_EPS) + decay * master)
    return (first_next, second_next, change)

def reference(tokens_in, doc_ids, out_grad, norm_gains, conv_taps, stream_weight, mixer_weight, hidden_weight, down_weight, gains_first, gains_second, taps_first, taps_second, stream_first, stream_second, mixer_first, mixer_second, hidden_first, hidden_second, down_first, down_second):
    valid = [doc_valid(doc_ids, offset) for offset in range(KERNEL)]

    def forward(tokens, gain_pair, tap_values, stream_w, mixer_w, hidden_w, down_w):
        return layer(tokens, gain_pair, tap_values, stream_w, mixer_w, hidden_w, down_w, valid)
    masters = (norm_gains.astype(jnp.float32), conv_taps.astype(jnp.float32), stream_weight.astype(jnp.float32), mixer_weight.astype(jnp.float32), hidden_weight.astype(jnp.float32), down_weight.astype(jnp.float32))
    block, pullback = jax.vjp(forward, tokens_in.astype(jnp.float32), masters[0], masters[1], masters[2], masters[3], masters[4], masters[5])
    grads = pullback(out_grad.astype(jnp.float32))
    square_total = jnp.float32(0.0)
    for gradient in grads[1:]:
        square_total = square_total + jnp.sum(gradient * gradient)
    grad_norm = jnp.sqrt(square_total)
    factor = jnp.minimum(1.0, CLIP_NORM / (grad_norm + 1e-06))
    firsts = (gains_first, taps_first, stream_first, mixer_first, hidden_first, down_first)
    seconds = (gains_second, taps_second, stream_second, mixer_second, hidden_second, down_second)
    decays = (0.0, DECAY_RATE, DECAY_RATE, DECAY_RATE, DECAY_RATE, DECAY_RATE)
    results = []
    for which in range(6):
        first_next, second_next, change = adam_step(masters[which], grads[which + 1], firsts[which], seconds[which], factor, decays[which])
        results.append((grads[which + 1], first_next, second_next, change))
    return (block.astype(jnp.bfloat16), grads[0], grad_norm, results[0][0], results[0][1], results[0][2], results[0][3], results[1][0], results[1][1], results[1][2], results[1][3], results[2][0], results[2][1], results[2][2], results[2][3], results[3][0], results[3][1], results[3][2], results[3][3], results[4][0], results[4][1], results[4][2], results[4][3], results[5][0], results[5][1], results[5][2], results[5][3])
```

```python
import functools
import jax
import jax.numpy as jnp
from jax import lax
from jax.experimental import pallas as pl
from jax.experimental.pallas import tpu as pltpu
from jax.sharding import PartitionSpec as P

EPS_NORM = 1e-05
LEARN_RATE = 0.02
BETA_FIRST = 0.5
BETA_SECOND = 0.5
CORRECTION = 1.0 - 0.5**3
ADAM_EPS = 1e-08
DECAY_RATE = 0.1
CLIP_NORM = 1.0


def shifted(value, axis, steps):
    count = lax.axis_size(axis)
    leading, last = (max(0, -steps), min(count, count - steps))
    return lax.ppermute(value, axis, [(source, source + steps) for source in range(leading, last)])


def rms_scale(values):
    return lax.rsqrt(jnp.mean(values * values, axis=-1, keepdims=True) + EPS_NORM)


def norm_back(grad_normed, normal, inverse, gain_row):
    scaled = grad_normed * gain_row
    return inverse * (scaled - normal * jnp.mean(scaled * normal, axis=-1, keepdims=True))


def adam_step(master, gradient, first_moment, second_moment, factor, decay):
    clipped = gradient * factor
    first_next = BETA_FIRST * first_moment + (1.0 - BETA_FIRST) * clipped
    second_next = BETA_SECOND * second_moment + (1.0 - BETA_SECOND) * clipped * clipped
    change = -LEARN_RATE * (
        first_next / CORRECTION / (jnp.sqrt(second_next / CORRECTION) + ADAM_EPS) + decay * master
    )
    return (first_next, second_next, change)


def contract_rows(left, right):
    return lax.dot_general(
        left, right, (((0,), (0,)), ((), ())), preferred_element_type=jnp.float32
    )


def contract_cols(left, right):
    return lax.dot_general(
        left, right, (((1,), (1,)), ((), ())), preferred_element_type=jnp.float32
    )


ROWS_STEP = 16
MESH = pl.DeviceIdType.MESH


def chain_kernel(axis, depth, finish, extra_in, extra_out, *refs):
    part_ref = refs[0]
    ins = refs[1 : 1 + extra_in]
    out_ref = refs[1 + extra_in]
    outs = refs[2 + extra_in : 2 + extra_in + extra_out]
    from_left, from_right, total, sums_send, sums_recv, back_send, back_recv = refs[
        2 + extra_in + extra_out :
    ]
    count = lax.axis_size(axis)
    me = lax.axis_index(axis)
    last = count - 1
    block = part_ref.shape[0] // count
    steps = block // depth
    ahead = min(1, steps)
    has_left = me > 0
    has_right = me < last

    def rows(which, step):
        return pl.ds(pl.multiple_of(which * block + step * depth, depth), depth)

    def inner(step):
        return pl.ds(pl.multiple_of(step * depth, depth), depth)

    def sum_copy(right, which, step, from_part):
        held = from_left if right else from_right
        source = part_ref.at[rows(which, step)] if from_part else held.at[which, inner(step)]
        lane = 0 if right else 1
        return pltpu.make_async_remote_copy(
            src_ref=source,
            dst_ref=held.at[which, inner(step)],
            send_sem=sums_send.at[lane, which, step],
            recv_sem=sums_recv.at[lane, which, step],
            device_id={axis: me + 1 if right else me - 1},
            device_id_type=MESH,
        )

    def back_copy(right, which, step):
        lane = 0 if right else 1
        place = out_ref.at[rows(which, step)]
        return pltpu.make_async_remote_copy(
            src_ref=place,
            dst_ref=place,
            send_sem=back_send.at[lane, which, step],
            recv_sem=back_recv.at[lane, which, step],
            device_id={axis: me + 1 if right else me - 1},
            device_id_type=MESH,
        )

    barrier = pltpu.get_barrier_semaphore()

    @pl.when(has_left)
    def _():
        pl.semaphore_signal(barrier, inc=1, device_id={axis: me - 1}, device_id_type=MESH)

    @pl.when(has_right)
    def _():
        pl.semaphore_signal(barrier, inc=1, device_id={axis: me + 1}, device_id_type=MESH)

    pl.semaphore_wait(barrier, jnp.where(has_left & has_right, 2, 1))

    def end_sends(step):
        for nth in range(last):
            @pl.when(me == 0)
            def _():
                sum_copy(True, last - nth, step, True).start()

            @pl.when(me == last)
            def _():
                sum_copy(False, nth, step, True).start()

    def pass_on(right, which, step):
        held = from_left if right else from_right
        sum_copy(right, which, step, False).wait_recv()
        place = (which, inner(step))
        added = held[place].astype(jnp.float32) + part_ref[rows(which, step)].astype(jnp.float32)
        held[place] = added.astype(held.dtype)
        sum_copy(right, which, step, False).start()

    def far_end(which):
        return jnp.maximum(which, last - which)

    def when_due(step, lag, allowed, action):
        due = step - lag

        @pl.when(allowed & (due >= 0) & (due < steps))
        def _():
            action(due)

    def total_up(step):
        total[...] = part_ref[rows(me, step)].astype(jnp.float32)

        @pl.when(has_left)
        def _():
            sum_copy(True, me, step, False).wait_recv()
            total[...] += from_left[me, inner(step)].astype(jnp.float32)

        @pl.when(has_right)
        def _():
            sum_copy(False, me, step, False).wait_recv()
            total[...] += from_right[me, inner(step)].astype(jnp.float32)

        out_ref[rows(me, step)] = finish(
            total[...], step, rows(me, step), inner(step), ins, outs
        ).astype(out_ref.dtype)

        @pl.when(has_right)
        def _():
            back_copy(True, me, step).start()

        @pl.when(has_left)
        def _():
            back_copy(False, me, step).start()

    def hand_on(right, which, step):
        back_copy(right, which, step).wait_recv()

        @pl.when(has_right if right else has_left)
        def _():
            back_copy(right, which, step).start()

    def one_step(step, carry):
        when_due(step, -ahead, step >= 0, end_sends)
        for nth in range(last):
            right_to, left_to = last - nth, nth
            when_due(
                step, me, has_left & (me < right_to), functools.partial(pass_on, True, right_to)
            )
            when_due(
                step, last - me, has_right & (me > left_to), functools.partial(pass_on, False, left_to)
            )
        when_due(step, far_end(me), step >= 0, total_up)
        for far in range(1, count):
            when_due(
                step,
                far_end(me - far) + far,
                me >= far,
                functools.partial(hand_on, True, me - far),
            )
            when_due(
                step,
                far_end(me + far) + far,
                me + far <= last,
                functools.partial(hand_on, False, me + far),
            )
        return carry

    for step in range(ahead):
        end_sends(step)
    lax.fori_loop(0, steps + 2 * last, one_step, 0)

    def sent(step, carry):
        for which in range(count):
            @pl.when(has_right & (me < which))
            def _():
                sum_copy(True, which, step, False).wait_send()

            @pl.when(has_left & (me > which))
            def _():
                sum_copy(False, which, step, False).wait_send()

            @pl.when(has_right & (me >= which))
            def _():
                back_copy(True, which, step).wait_send()

            @pl.when(has_left & (me <= which))
            def _():
                back_copy(False, which, step).wait_send()

        return carry

    lax.fori_loop(0, steps, sent, 0)


def chain_sum(part, ins, finish, extra_outs, number, axis="tensor"):
    count = lax.axis_size(axis)
    tokens, width = part.shape
    block = tokens // count
    depth = min(ROWS_STEP, block)
    steps = block // depth
    vmem = pl.BlockSpec(memory_space=pltpu.VMEM)
    return pl.pallas_call(
        functools.partial(chain_kernel, axis, depth, finish, len(ins), len(extra_outs)),
        out_shape=[jax.ShapeDtypeStruct((tokens, width), jnp.bfloat16)] + list(extra_outs),
        in_specs=[vmem] * (1 + len(ins)),
        out_specs=[vmem] * (1 + len(extra_outs)),
        scratch_shapes=[
            pltpu.VMEM((count, block, width), jnp.bfloat16),
            pltpu.VMEM((count, block, width), jnp.bfloat16),
            pltpu.VMEM((depth, width), jnp.float32),
            pltpu.SemaphoreType.DMA((2, count, steps)),
            pltpu.SemaphoreType.DMA((2, count, steps)),
            pltpu.SemaphoreType.DMA((2, count, steps)),
            pltpu.SemaphoreType.DMA((2, count, steps)),
        ],
        compiler_params=pltpu.CompilerParams(collective_id=number, has_side_effects=True),
        name="chain_sum_%d" % number,
    )(part, *ins)


def finish_middle(total, step, whole, own, ins, outs):
    tokens_ref, gain_ref = ins
    (middle_ref,) = outs
    middle = tokens_ref[whole].astype(jnp.float32) + total
    middle_ref[own] = middle
    return middle * rms_scale(middle) * gain_ref[...]


def finish_feed(total, step, whole, own, ins, outs):
    (middle_ref,) = ins
    return middle_ref[own] + total


def add_gain(gain_ref, step, addend):
    summed = jnp.sum(addend, axis=0, keepdims=True)

    @pl.when(step == 0)
    def _():
        gain_ref[...] = summed

    @pl.when(step > 0)
    def _():
        gain_ref[...] += summed


def finish_middle_back(total, step, whole, own, ins, outs):
    middle_ref, upstream_ref, gain_ref = ins
    back_ref, gain_grad_ref = outs
    middle = middle_ref[own]
    inverse = rms_scale(middle)
    normal = middle * inverse
    add_gain(gain_grad_ref, step, total * normal)
    back = upstream_ref[whole].astype(jnp.float32) + norm_back(
        total, normal, inverse, gain_ref[...]
    )
    back_ref[own] = back
    return back


def finish_input_back(total, step, whole, own, ins, outs):
    tokens_ref, middle_back_ref, gain_ref = ins
    (gain_grad_ref,) = outs
    tokens = tokens_ref[whole].astype(jnp.float32)
    inverse = rms_scale(tokens)
    normal = tokens * inverse
    add_gain(gain_grad_ref, step, total * normal)
    return middle_back_ref[own] + norm_back(total, normal, inverse, gain_ref[...])


def over_dp(grad):
    return lax.psum_scatter(grad.astype(jnp.bfloat16), "dp", scatter_dimension=0, tiled=True)


def own_columns(weight, share):
    return lax.dynamic_slice_in_dim(weight, lax.axis_index("dp") * share, share, 1)


LANES = 128


def tail_kernel(*refs):
    gain_refs, taps_ref, share_refs = refs[0:2], refs[2], refs[3:8]
    gains_ref, taps_sum_ref, stats_ref = refs[8:11]
    mine, slots, joint, joint_slots, send_dp, recv_dp, send_tensor, recv_tensor = refs[11:]
    many = lax.axis_size("dp")
    few = lax.axis_size("tensor")
    place = lax.axis_index("dp")
    level = lax.axis_index("tensor")
    width = gains_ref.shape[1]
    spans = width // LANES
    tap_count, tap_width = taps_ref.shape
    tap_spans = tap_width // LANES
    tap_start = 2 * spans
    square_row = tap_start + tap_count * tap_spans

    def peer_dp(away):
        return lax.rem(place + away, many)

    def peer_tensor(away):
        return lax.rem(level + away, few)

    def copy_dp(away, slot):
        return pltpu.make_async_remote_copy(
            src_ref=mine,
            dst_ref=slots.at[slot],
            send_sem=send_dp.at[away],
            recv_sem=recv_dp.at[slot],
            device_id={"dp": peer_dp(away)},
            device_id_type=MESH,
        )

    def copy_tensor(away, slot):
        return pltpu.make_async_remote_copy(
            src_ref=joint,
            dst_ref=joint_slots.at[slot],
            send_sem=send_tensor.at[away],
            recv_sem=recv_tensor.at[slot],
            device_id={"tensor": peer_tensor(away)},
            device_id_type=MESH,
        )

    barrier = pltpu.get_barrier_semaphore()

    def greet_dp(away, carry):
        pl.semaphore_signal(barrier, inc=1, device_id={"dp": peer_dp(away)}, device_id_type=MESH)
        return carry

    def greet_tensor(away, carry):
        pl.semaphore_signal(
            barrier, inc=1, device_id={"tensor": peer_tensor(away)}, device_id_type=MESH
        )
        return carry

    lax.fori_loop(1, many, greet_dp, 0)
    lax.fori_loop(1, few, greet_tensor, 0)
    mine[...] = jnp.zeros_like(mine)
    for which in range(2):
        for span in range(spans):
            mine[pl.ds(which * spans + span, 1)] = gain_refs[which][:, span * LANES : (span + 1) * LANES]
    for tap in range(tap_count):
        for span in range(tap_spans):
            mine[pl.ds(tap_start + tap * tap_spans + span, 1)] = taps_ref[
                tap : tap + 1, span * LANES : (span + 1) * LANES
            ]
    square = jnp.zeros((1, 1), jnp.float32)
    for share_ref in share_refs:
        share = share_ref[...].astype(jnp.float32)
        square = square + jnp.sum(
            jnp.sum(share * share, axis=0, keepdims=True), axis=1, keepdims=True
        )
    first = lax.broadcasted_iota(jnp.int32, (1, LANES), 1) == 0
    mine[pl.ds(square_row, 1)] = jnp.where(first, square, 0.0)
    pl.semaphore_wait(barrier, many + few - 2)

    def start_dp(away, carry):
        copy_dp(away, place).start()
        return carry

    def await_dp(away, carry):
        copy_dp(away, lax.rem(place + many - away, many)).wait_recv()
        return carry

    lax.fori_loop(1, many, start_dp, 0)
    slots[place] = mine[...]
    lax.fori_loop(1, many, await_dp, 0)
    joint[...] = lax.fori_loop(
        1, many, lambda slot, summed: summed + slots[slot], slots[0]
    )
    taps = joint[pl.ds(tap_start, tap_count * tap_spans)]
    tap_square = jnp.sum(jnp.sum(taps * taps, axis=0, keepdims=True), axis=1, keepdims=True)
    joint[pl.ds(square_row, 1)] += jnp.where(first, tap_square, 0.0)
    for tap in range(tap_count):
        for span in range(tap_spans):
            taps_sum_ref[tap : tap + 1, span * LANES : (span + 1) * LANES] = joint[
                pl.ds(tap_start + tap * tap_spans + span, 1)
            ]
    for away in range(1, few):
        copy_tensor(away, level).start()
    joint_slots[level] = joint[...]
    for away in range(1, few):
        copy_tensor(away, lax.rem(level + few - away, few)).wait_recv()
    summed = joint_slots[0]
    for slot in range(1, few):
        summed = summed + joint_slots[slot]
    mine_gains = summed[:tap_start]
    gain_square = jnp.sum(
        jnp.sum(mine_gains * mine_gains, axis=0, keepdims=True), axis=1, keepdims=True
    )
    row = summed[square_row : square_row + 1]
    norm = jnp.sqrt(jnp.sum(row, axis=1, keepdims=True) + gain_square)
    stats_ref[0:1] = jnp.broadcast_to(norm, (1, LANES))
    stats_ref[1:2] = jnp.broadcast_to(
        jnp.minimum(1.0, CLIP_NORM / (norm + 1e-06)), (1, LANES)
    )
    for which in range(2):
        for span in range(spans):
            start = which * spans + span
            gains_ref[which : which + 1, span * LANES : (span + 1) * LANES] = summed[
                start : start + 1
            ]

    def sent_dp(away, carry):
        copy_dp(away, place).wait_send()
        return carry

    lax.fori_loop(1, many, sent_dp, 0)
    for away in range(1, few):
        copy_tensor(away, level).wait_send()


def tail_sums(gain_parts, taps_part, shares, number):
    many, few = lax.axis_size("dp"), lax.axis_size("tensor")
    width = gain_parts[0].shape[1]
    rows = (2 * width + taps_part.size) // LANES + 1
    rows = -(-rows // 8) * 8
    vmem = pl.BlockSpec(memory_space=pltpu.VMEM)
    return pl.pallas_call(
        tail_kernel,
        out_shape=[
            jax.ShapeDtypeStruct((2, width), jnp.float32),
            jax.ShapeDtypeStruct(taps_part.shape, jnp.float32),
            jax.ShapeDtypeStruct((2, LANES), jnp.float32),
        ],
        in_specs=[vmem] * (3 + len(shares)),
        out_specs=[vmem] * 3,
        scratch_shapes=[
            pltpu.VMEM((rows, LANES), jnp.float32),
            pltpu.VMEM((many, rows, LANES), jnp.float32),
            pltpu.VMEM((rows, LANES), jnp.float32),
            pltpu.VMEM((few, rows, LANES), jnp.float32),
            pltpu.SemaphoreType.DMA((many,)),
            pltpu.SemaphoreType.DMA((many,)),
            pltpu.SemaphoreType.DMA((few,)),
            pltpu.SemaphoreType.DMA((few,)),
        ],
        compiler_params=pltpu.CompilerParams(collective_id=number, has_side_effects=True),
        name="tail_sums",
    )(*gain_parts, taps_part, *shares)


def adam_kernel(decay, counts, place_ref, stats_ref, *refs):
    grads, (weight_ref, first_ref, second_ref) = refs[:counts], refs[counts : counts + 3]
    grad_ref, first_next_ref, second_next_ref, step_ref = refs[counts + 3 :]
    factor = stats_ref[1:2, 0:1]

    def update(source):
        shape = grad_ref.shape
        grad = source[...].astype(jnp.float32).reshape(shape)
        master = weight_ref[...].astype(jnp.float32).reshape(shape)
        first_next, second_next, change = adam_step(
            master, grad, first_ref[...], second_ref[...], factor, decay
        )
        grad_ref[...] = grad
        first_next_ref[...] = first_next
        second_next_ref[...] = second_next
        step_ref[...] = change

    if counts == 1:
        update(grads[0])
    else:
        for which in range(counts):
            @pl.when(pl.program_id(0) == which)
            def _():
                update(grads[which])


def adam_call(grid, grads, grad_specs, weight, weight_spec, first, second, spec, stats, place, decay):
    return pl.pallas_call(
        functools.partial(adam_kernel, decay, len(grads)),
        grid_spec=pltpu.PrefetchScalarGridSpec(
            num_scalar_prefetch=1,
            grid=grid,
            in_specs=[pl.BlockSpec(stats.shape, lambda *_: (0, 0))]
            + grad_specs
            + [weight_spec, spec, spec],
            out_specs=[spec] * 4,
        ),
        out_shape=[jax.ShapeDtypeStruct(first.shape, jnp.float32)] * 4,
        name="adam",
    )(place, stats, *grads, weight, first, second)


def adam_stacked(grads, weight, first, second, stats, place, pieces):
    stack, share, width = first.shape
    depth = share // pieces
    grad_specs = (
        [pl.BlockSpec((depth, width), lambda which, piece, _: (piece, which))]
        if len(grads) == 1
        else [
            pl.BlockSpec(
                (depth, width),
                lambda which, piece, _, own=own: (
                    jnp.where(which == own, piece, jnp.where(which < own, 0, pieces - 1)),
                    0,
                ),
            )
            for own in range(len(grads))
        ]
    )
    return adam_call(
        (stack, pieces),
        grads,
        grad_specs,
        weight,
        pl.BlockSpec(
            (1, depth, width), lambda which, piece, place: (which, place[0] * pieces + piece, 0)
        ),
        first,
        second,
        pl.BlockSpec((1, depth, width), lambda which, piece, _: (which, piece, 0)),
        stats,
        place,
        DECAY_RATE,
    )


def adam_flat(grad, weight, first, second, stats, place, pieces, decay):
    rows, width = first.shape
    spec = pl.BlockSpec((rows // pieces, width), lambda piece, _: (piece, 0))
    return adam_call(
        (pieces,), [grad], [spec], weight, spec, first, second, spec, stats, place, decay
    )


def body(
    tokens_in,
    doc_ids,
    out_grad,
    norm_gains,
    conv_taps,
    stream_weight,
    mixer_weight,
    hidden_weight,
    down_weight,
    gains_first,
    gains_second,
    taps_first,
    taps_second,
    stream_first,
    stream_second,
    mixer_first,
    mixer_second,
    hidden_first,
    hidden_second,
    down_first,
    down_second,
):
    tok_rows = tokens_in.shape[0]
    kernel = conv_taps.shape[0]
    reach = kernel - 1
    first_row = lax.axis_index("dp") * tok_rows
    filler = jnp.full((reach,), -1, jnp.int32)
    padded_ids = jnp.concatenate([filler, doc_ids, filler])
    window = lax.dynamic_slice_in_dim(padded_ids, first_row, tok_rows + 2 * reach)
    current = window[reach : reach + tok_rows]
    back_valid = [
        (window[reach - offset : reach - offset + tok_rows] == current).astype(jnp.float32)[:, None]
        for offset in range(kernel)
    ]
    ahead_valid = [
        (window[reach + offset : reach + offset + tok_rows] == current).astype(jnp.float32)[:, None]
        for offset in range(kernel)
    ]
    tokens = tokens_in.astype(jnp.float32)
    gain_pair = norm_gains.astype(jnp.float32)
    tap_values = conv_taps.astype(jnp.float32)
    scale_one = rms_scale(tokens)
    normal_one = tokens * scale_one
    normed_one = (normal_one * gain_pair[0]).astype(jnp.bfloat16)
    streams = jnp.einsum(
        "td,sdc->stc", normed_one, stream_weight, preferred_element_type=jnp.float32
    )
    product = (streams[0] * streams[2]).astype(jnp.bfloat16)
    edge_rows = shifted(product[tok_rows - reach :], "dp", 1)
    extended = jnp.concatenate([edge_rows, product], 0).astype(jnp.float32)
    conv_out = tap_values[0] * extended[reach : reach + tok_rows] * back_valid[0]
    for offset in range(1, kernel):
        conv_out = (
            conv_out
            + tap_values[offset]
            * extended[reach - offset : reach - offset + tok_rows]
            * back_valid[offset]
        )
    gated_rows = (streams[1] * conv_out).astype(jnp.bfloat16)
    branch_part = jnp.dot(gated_rows, mixer_weight, preferred_element_type=jnp.float32)
    width = tokens_in.shape[1]
    count = lax.axis_size("tensor")
    own_rows = jax.ShapeDtypeStruct((tok_rows // count, width), jnp.float32)
    gain_row = jax.ShapeDtypeStruct((1, width), jnp.float32)
    normed_two, middle = chain_sum(
        branch_part.astype(jnp.bfloat16), [tokens_in, gain_pair[1:2]], finish_middle, [own_rows], 1
    )
    gate, up = (
        jnp.dot(normed_two, hidden_weight[which], preferred_element_type=jnp.float32)
        for which in range(2)
    )
    sigmoid_gate = jax.nn.sigmoid(gate)
    silu_gate = gate * sigmoid_gate
    active = (silu_gate * up).astype(jnp.bfloat16)
    grad_active = contract_cols(out_grad, down_weight)
    grad_gate = (
        grad_active * up * sigmoid_gate * (1.0 + gate * (1.0 - sigmoid_gate))
    ).astype(jnp.bfloat16)
    grad_up = (grad_active * silu_gate).astype(jnp.bfloat16)
    normed_two_part = contract_cols(grad_gate, hidden_weight[0]) + contract_cols(
        grad_up, hidden_weight[1]
    )
    feed_part = jnp.dot(active, down_weight, preferred_element_type=jnp.float32)
    down_share = over_dp(contract_rows(out_grad, active))
    gate_share = over_dp(contract_rows(normed_two, grad_gate))
    up_share = over_dp(contract_rows(normed_two, grad_up))
    grad_branch, grad_middle, gain_two_part = chain_sum(
        normed_two_part.astype(jnp.bfloat16),
        [middle, out_grad, gain_pair[1:2]],
        finish_middle_back,
        [own_rows, gain_row],
        2,
    )
    (block_out,) = chain_sum(feed_part.astype(jnp.bfloat16), [middle], finish_feed, [], 3)
    mixer_part = contract_rows(grad_branch, gated_rows)
    grad_gated = contract_cols(grad_branch, mixer_weight)
    grad_c = grad_gated * conv_out
    grad_conv = (grad_gated * streams[1]).astype(jnp.bfloat16)
    ahead_rows = shifted(grad_conv[:reach], "dp", -1)
    trailing = jnp.concatenate([grad_conv, ahead_rows], 0).astype(jnp.float32)
    grad_conv_wide = trailing[:tok_rows]
    taps_part = jnp.stack(
        [
            jnp.sum(
                grad_conv_wide
                * extended[reach - offset : reach - offset + tok_rows]
                * back_valid[offset],
                axis=0,
            )
            for offset in range(kernel)
        ]
    )
    grad_product = tap_values[0] * grad_conv_wide * ahead_valid[0]
    for offset in range(1, kernel):
        grad_product = (
            grad_product
            + tap_values[offset] * trailing[offset : offset + tok_rows] * ahead_valid[offset]
        )
    grad_streams = jnp.stack([grad_product * streams[2], grad_c, grad_product * streams[0]]).astype(
        jnp.bfloat16
    )
    normed_one_part = jnp.einsum(
        "stc,sdc->td", grad_streams, stream_weight, preferred_element_type=jnp.float32
    )
    mixer_share = over_dp(mixer_part)
    stream_cols = jnp.concatenate(
        [contract_rows(normed_one, grad_streams[which]) for which in range(3)], 1
    )
    stream_share = over_dp(stream_cols)
    input_back, gain_one_part = chain_sum(
        normed_one_part.astype(jnp.bfloat16),
        [tokens_in, grad_middle, gain_pair[0:1]],
        finish_input_back,
        [gain_row],
        4,
    )
    input_grad = input_back.astype(jnp.float32)
    gains_sum, taps_sum, stats = tail_sums(
        [gain_one_part, gain_two_part],
        taps_part,
        [stream_share, mixer_share, gate_share, up_share, down_share],
        5,
    )
    grad_norm = stats[0, 0]
    place = lax.axis_index("dp").astype(jnp.int32)[None]
    gains_out = adam_flat(
        gains_sum, norm_gains, gains_first, gains_second, stats, place, 1, 0.0
    )
    taps_out = adam_flat(
        taps_sum, conv_taps, taps_first, taps_second, stats, place, 1, DECAY_RATE
    )
    stream_out = adam_stacked(
        [stream_share], stream_weight, stream_first, stream_second, stats, place, 1
    )
    mixer_out = adam_flat(
        mixer_share.T,
        own_columns(mixer_weight, mixer_first.shape[1]),
        mixer_first,
        mixer_second,
        stats,
        place,
        1,
        DECAY_RATE,
    )
    hidden_out = adam_stacked(
        [gate_share, up_share], hidden_weight, hidden_first, hidden_second, stats, place, 3
    )
    down_out = adam_flat(
        down_share.T,
        own_columns(down_weight, down_first.shape[1]),
        down_first,
        down_second,
        stats,
        place,
        6,
        DECAY_RATE,
    )
    return (
        block_out,
        input_grad,
        grad_norm,
        *gains_out,
        *taps_out,
        *stream_out,
        *mixer_out,
        *hidden_out,
        *down_out,
    )


def solution(mesh):
    return jax.shard_map(
        body,
        mesh=mesh,
        in_specs=(
            P("dp", None),
            P(),
            P("dp", None),
            P(),
            P(None, "tensor"),
            P(None, None, "tensor"),
            P("tensor", None),
            P(None, None, "tensor"),
            P("tensor", None),
            P(),
            P(),
            P(None, "tensor"),
            P(None, "tensor"),
            P(None, "dp", "tensor"),
            P(None, "dp", "tensor"),
            P("tensor", "dp"),
            P("tensor", "dp"),
            P(None, "dp", "tensor"),
            P(None, "dp", "tensor"),
            P("tensor", "dp"),
            P("tensor", "dp"),
        ),
        out_specs=(
            P("dp", None),
            P("dp", None),
            P(),
            P(),
            P(),
            P(),
            P(),
            P(None, "tensor"),
            P(None, "tensor"),
            P(None, "tensor"),
            P(None, "tensor"),
            P(None, "dp", "tensor"),
            P(None, "dp", "tensor"),
            P(None, "dp", "tensor"),
            P(None, "dp", "tensor"),
            P("tensor", "dp"),
            P("tensor", "dp"),
            P("tensor", "dp"),
            P("tensor", "dp"),
            P(None, "dp", "tensor"),
            P(None, "dp", "tensor"),
            P(None, "dp", "tensor"),
            P(None, "dp", "tensor"),
            P("tensor", "dp"),
            P("tensor", "dp"),
            P("tensor", "dp"),
            P("tensor", "dp"),
        ),
        check_vma=False,
    )
```
